32 devices in a mesh: groups: 2 (over y), mp: 2 (over x), expert: 4 (over z), dp: 2 (over core).
Axes of the slice: x: 2, y: 2, z: 4, core: 2. Of those that a mesh axis runs over, the one named last changes fastest.
Arguments:
- hidden_in: bfloat16 [1024, 4096], P(('groups', 'expert', 'dp'), 'mp'), parts along dimension 0, may hold values from -6 to 6
- norm_gain: bfloat16 [2, 4096], P(None, 'mp'), may hold values from 0.25 to 1.75
- expert_ids: int32 [2, 1024, 2], P(None, ('groups', 'expert', 'dp')), parts along dimension 1, may hold values from 0 to 3, all different within a row; in each aligned block of 64 rows (0 to 63, 64 to 127, ..., all dimensions but the last counted through in order) at most 64 rows name the same one
- gate_counts: int32 [2, 1024, 2], P(None, ('groups', 'expert', 'dp')), parts along dimension 1, may hold values from 8 to 15
- exit_layer: int32 [1024], P(('groups', 'expert', 'dp')), parts along dimension 0, may hold values from 1 to 2
- w_gate: bfloat16 [2, 4, 7168, 4096], P(None, 'expert', ('mp', 'dp')), may hold values from -0.09375 to 0.09375
- w_up: bfloat16 [2, 4, 7168, 4096], P(None, 'expert', ('mp', 'dp')), may hold values from -0.09375 to 0.09375
- w_down: bfloat16 [2, 4, 7168, 4096], P(None, 'expert', ('mp', 'dp')), may hold values from -0.0625 to 0.0625
Outputs:
- hidden_out: bfloat16 [1024, 4096], P(('groups', 'expert', 'dp'), 'mp'), parts along dimension 0
The draws below stay inside these ranges and needn't reach their ends.
There are 2 independent parts, one for each index of `groups`. The reference program is written for one: setup_inputs(seed, part) draws one part's arguments, and reference() takes and returns one part's arrays. A program takes and returns all parts, laid end to end along the dimension named above; an argument that names none is the same for every part. Nothing has to cross between parts.
Inputs may be any that keep to these rules, and one draw needn't show every extreme that they name: `expert_ids`: A token's two ids in a layer differ. In the rows of one device in one layer (aligned blocks of 64 rows, layer by layer) some expert may be named by all 64 rows.
All inputs are finite; a program needn't handle non-finite values.
Results may differ from the reference program's by a relative error of at most 0.014.
Values may be sent and summed in bfloat16 or wider, within the bound.
A program may use at most 384 MiB of HBM per device.

```python
import math
import jax
import jax.numpy as jnp
import numpy as np
from jax import lax

D = 4096
FF = 7168
LAYERS = 2
TOK_DEV = 64
EXPERTS = 4
TOKENS = 512
N_MP = 2


def draw_exit_layer(key, part):
    own_key = jax.random.fold_in(key, 17)
    key_roll, key_early = jax.random.split(own_key)
    roll_value = jax.random.randint(key_roll, (TOKENS,), 0, 100)
    early_exit = jax.random.randint(key_early, (TOKENS,), 1, max(LAYERS, 2))
    exits = jnp.where(roll_value < 95, LAYERS, early_exit)
    position = jnp.arange(TOKENS)
    exits = jnp.where(position == 0, 1, jnp.where(position == 1, LAYERS, exits))
    return exits.astype(jnp.int32)


def place_ends(array, stream_key, least, largest):
    place = [jax.random.randint(jax.random.fold_in(stream_key, axis), (), 0, length) for axis, length in enumerate(array.shape)]
    main_axis = array.shape.index(max(array.shape))
    beside = place[:main_axis] + [(place[main_axis] + 1) % array.shape[main_axis]] + place[main_axis + 1:]
    return array.at[tuple(place)].set(least).at[tuple(beside)].set(largest)


def shard_levels(rng, dims, cuts, smallest, high):
    def one(dim, parts):
        steps = jax.random.uniform(jax.random.fold_in(jax.random.fold_in(rng, 6), dim), (parts,), jnp.float32, smallest / len(cuts), high / len(cuts))
        return jnp.repeat(jnp.exp(steps), dims[dim] // parts).reshape((-1,) + (1,) * (len(dims) - dim - 1))

    loudness = one(*cuts[0])
    for cut in cuts[1:]:
        loudness = loudness * one(*cut)
    return loudness


def routed_block(key, own, number, rows, amount, top, limit, skew):
    order = jax.random.permutation(key, amount)
    packed, ordinary = portions_of(amount, rows * top, limit, skew, True), portions_of(amount, rows * top, limit, skew, False)
    places = jnp.arange(amount)

    def named(sizes, turn):
        used = int((sizes > 0).sum())
        fixed = max(1, used // 4)
        shifted = fixed + (places - fixed + turn * (used - fixed)) % max(1, amount - fixed)
        return jnp.zeros((amount,), jnp.int32).at[order[jnp.where(places < fixed, places, shifted)]].set(jnp.asarray(sizes, jnp.int32))

    sizes = jnp.where(number % 4 == 0, named(packed, number // 4), named(ordinary, number - number // 4 - 1))
    mixed = jax.random.permutation(jax.random.fold_in(own, 3), amount)
    source_of, taker = mixed[0:amount // 2 * 2:2], mixed[1:amount // 2 * 2:2]
    slack = jnp.minimum(sizes[source_of] - 1, limit - sizes[taker]) // 2
    slack = jnp.where((source_of == order[0]) | (taker == order[0]) | (sizes[taker] == 0), 0, jnp.maximum(slack, 0))
    shifted = jax.random.randint(jax.random.fold_in(own, 4), (amount // 2,), 0, 1 << 20) % (slack + 1)
    sizes = sizes.at[source_of].add(-shifted).at[taker].add(shifted)
    members = jnp.searchsorted(jnp.cumsum(sizes), jnp.arange(rows * top), side="right").astype(jnp.int32)
    table = members.reshape(top, rows).T
    table = table[jax.random.permutation(jax.random.fold_in(own, 1), rows)]
    turn = jax.random.randint(jax.random.fold_in(own, 2), (rows, 1), 0, top)
    return jnp.take_along_axis(table, (jnp.arange(top)[None, :] + turn) % top, axis=1)


def portions_of(count, total, reach, lean, full):
    portions = [(1 << 20) // math.isqrt(standing ** lean) + 1 for standing in range(1, count + 1)]
    largest = reach if full else min(reach, max(-(-total // count), total * portions[0] // sum(portions)))
    least = 1 if total - largest >= count - 1 else 0
    holding, surplus = [largest] + [least] * (count - 1), total - largest - least * (count - 1)
    while surplus > 0:
        free = [i for i in range(1, count) if holding[i] < largest] or [i for i in range(1, count) if holding[i] < reach]
        whole, left = sum([portions[i] for i in free]), surplus
        for i in free:
            more = min(reach - holding[i], max(1, left * portions[i] // whole), surplus)
            holding[i] = holding[i] + more
            surplus = surplus - more
    return np.array(holding)


def centred(key, shape, deviation, most, pieces=(), held_as=jnp.bfloat16):
    drawn = jax.random.normal(key, shape, jnp.float32) * deviation
    if len(pieces) > 0:
        drawn = shard_levels(key, shape, pieces, -0.22, 0.18) * drawn
    return jnp.clip(drawn, min=-most, max=most).astype(held_as)


def setup_inputs(seed: int = 0, part: int = 0) -> dict:
    key_of = jax.random.split(jax.random.key(seed), 9)
    own_keys = jax.random.split(jax.random.fold_in(key_of[8], part), 9)
    hidden_in = centred(own_keys[0], (TOKENS, D), 1.0, 6.0, ((0, 8), (1, 2)))
    norm_gain = jnp.clip(1.0 + 0.15 * jax.random.normal(key_of[1], (LAYERS, D), jnp.float32), 0.25, 1.75).astype(jnp.bfloat16)
    expert_ids_keys = jax.random.split(jax.random.fold_in(own_keys[2], 1), LAYERS * TOKENS // TOK_DEV)
    expert_ids_turns = jax.random.permutation(jax.random.fold_in(own_keys[2], 3), LAYERS * TOKENS // TOK_DEV)
    expert_ids = jax.vmap(lambda own, number: routed_block(jax.random.fold_in(own_keys[2], 2), own, number, TOK_DEV, EXPERTS, 2, TOK_DEV, 2))(expert_ids_keys, expert_ids_turns).reshape((LAYERS, TOKENS, 2))
    gate_counts = place_ends(jax.random.randint(own_keys[3], (LAYERS, TOKENS, 2), 8, 16), jax.random.fold_in(own_keys[3], 1), 8, 15).astype(jnp.int32)
    exit_layer = draw_exit_layer(jax.random.fold_in(jax.random.fold_in(key_of[8], part), 71), part)
    w_gate = centred(key_of[5], (LAYERS, EXPERTS, FF, D), D ** -0.5, 0.09375, ((1, 4), (2, 4)))
    w_up = centred(key_of[6], (LAYERS, EXPERTS, FF, D), D ** -0.5, 0.09375, ((1, 4), (2, 4)))
    w_down = centred(key_of[7], (LAYERS, EXPERTS, FF, D), FF ** -0.5, 0.0625, ((1, 4), (2, 4)))
    return {"hidden_in": hidden_in, "norm_gain": norm_gain, "expert_ids": expert_ids, "gate_counts": gate_counts, "exit_layer": exit_layer, "w_gate": w_gate, "w_up": w_up, "w_down": w_down}


norm_floor = 0.1

def expert_output(normed, gate_rows, up_rows, down_rows):
    contract = (((1,), (1,)), ((), ()))
    gate_val = lax.dot_general(normed, gate_rows, contract, preferred_element_type=jnp.float32)
    up_val = lax.dot_general(normed, up_rows, contract, preferred_element_type=jnp.float32)
    hidden = (jax.nn.silu(gate_val) * up_val).astype(jnp.bfloat16)
    block_len = FF // N_MP
    running = jnp.zeros((normed.shape[0], D), jnp.float32)
    for block_idx in range(N_MP):
        row_start = block_idx * block_len
        partial_value = jnp.dot(hidden[:, row_start:row_start + block_len], down_rows[row_start:row_start + block_len], preferred_element_type=jnp.float32)
        rounded = lax.optimization_barrier(partial_value.astype(jnp.bfloat16))
        running = running + rounded.astype(jnp.float32)
    return running.astype(jnp.bfloat16)

def reference(hidden_in, norm_gain, expert_ids, gate_counts, exit_layer, w_gate, w_up, w_down):
    current = hidden_in
    expert_range = jnp.arange(EXPERTS, dtype=jnp.int32)
    for layer_idx in range(LAYERS):
        current_f32 = current.astype(jnp.float32)
        sum_squares = lax.optimization_barrier(jnp.sum(current_f32 * current_f32, axis=1, keepdims=True))
        inv_rms = lax.rsqrt(sum_squares / D + norm_floor)
        normed = (current_f32 * inv_rms * norm_gain[layer_idx].astype(jnp.float32)[None, :]).astype(jnp.bfloat16)
        outputs = lax.map(lambda weights: expert_output(normed, weights[0], weights[1], weights[2]), (w_gate[layer_idx], w_up[layer_idx], w_down[layer_idx]))
        counts = gate_counts[layer_idx].astype(jnp.float32)
        gate_share = counts / lax.optimization_barrier(jnp.sum(counts, axis=1, keepdims=True))
        matched = expert_ids[layer_idx][:, :, None] == expert_range[None, None, :]
        weight_te = lax.optimization_barrier(jnp.sum(jnp.where(matched, gate_share[:, :, None], jnp.float32(0.0)), axis=1))
        active = (exit_layer > layer_idx).astype(jnp.float32)
        weight_te = weight_te * active[:, None]
        update = jnp.einsum('te,etd->td', weight_te, outputs.astype(jnp.float32), precision=lax.Precision.HIGHEST)
        current = (current_f32 + update).astype(jnp.bfloat16)
    return current
```

```python
import jax
import jax.numpy as jnp
from jax import lax
from jax.sharding import PartitionSpec as P

LAYERS = 2


norm_floor = 0.1


def body(hidden_in, norm_gain, expert_ids, gate_counts, exit_layer, w_gate, w_up, w_down):
    experts = lax.axis_size("expert")
    shards = lax.axis_size("mp")
    full_width = hidden_in.shape[1] * shards
    contract = (((1,), (1,)), ((), ()))
    expert_range = jnp.arange(experts, dtype=jnp.int32)
    counts = gate_counts.astype(jnp.float32)
    gate_share = counts / jnp.sum(counts, axis=2, keepdims=True)
    active = exit_layer[None, :] > jnp.arange(LAYERS, dtype=jnp.int32)[:, None]
    matched = (expert_ids[..., None] == expert_range) & active[:, :, None, None]
    weight = jnp.sum(jnp.where(matched, gate_share[..., None], jnp.float32(0.0)), axis=2)
    weight = lax.all_gather(weight, ("expert", "dp"), axis=1, tiled=True)
    weight = lax.dynamic_index_in_dim(weight, lax.axis_index("expert"), 2, keepdims=True)
    gain = lax.all_gather(norm_gain, "mp", axis=1, tiled=True).astype(jnp.float32)
    current = hidden_in
    for layer_idx in range(LAYERS):
        rows = lax.all_gather(current, "mp", axis=1, tiled=True)
        rows_f32 = rows.astype(jnp.float32)
        inv_rms = lax.rsqrt(jnp.sum(rows_f32 * rows_f32, axis=1) / full_width + norm_floor)
        normed = (rows_f32 * inv_rms[:, None] * gain[layer_idx][None, :]).astype(jnp.bfloat16)
        inputs = lax.all_gather(normed, ("expert", "dp"), axis=0, tiled=True)
        gate_val = lax.dot_general(
            inputs, w_gate[layer_idx, 0], contract, preferred_element_type=jnp.float32
        )
        up_val = lax.dot_general(
            inputs, w_up[layer_idx, 0], contract, preferred_element_type=jnp.float32
        )
        hidden = (jax.nn.silu(gate_val) * up_val * weight[layer_idx]).astype(jnp.bfloat16)
        partial_value = jnp.dot(
            hidden, w_down[layer_idx, 0], preferred_element_type=jnp.float32
        ).astype(jnp.bfloat16)
        summed = lax.psum_scatter(
            partial_value, ("expert", "dp"), scatter_dimension=0, tiled=True
        )
        summed = lax.psum_scatter(summed, "mp", scatter_dimension=1, tiled=True)
        current = (current.astype(jnp.float32) + summed.astype(jnp.float32)).astype(jnp.bfloat16)
    return current


def solution(mesh):
    in_specs = (
        P(("groups", "expert", "dp"), "mp"),
        P(None, "mp"),
        P(None, ("groups", "expert", "dp"), None),
        P(None, ("groups", "expert", "dp"), None),
        P(("groups", "expert", "dp")),
        P(None, "expert", ("mp", "dp"), None),
        P(None, "expert", ("mp", "dp"), None),
        P(None, "expert", ("mp", "dp"), None),
    )
    out_specs = P(("groups", "expert", "dp"), "mp")
    return jax.shard_map(body, mesh=mesh, in_specs=in_specs, out_specs=out_specs, check_vma=False)
```

```python
import functools

import jax
import jax.numpy as jnp
from jax import lax
from jax.experimental import pallas as pl
from jax.experimental.pallas import tpu as pltpu
from jax.sharding import PartitionSpec as P

LAYERS = 2


norm_floor = 0.1
MESH = pl.DeviceIdType.MESH
CHUNK = 16


def tile_of(length, best):
    tile = best
    while tile >= 128:
        if length % tile == 0:
            return tile
        tile //= 2
    return length


def layer_kernel(
    layer_idx, n, dp, mp,
    cur_ref, gain_ref, share_ref, wg_hbm, wu_hbm, wd_hbm, out_ref,
    wg, wu, wd, x, p, rd, rcw, rcc, xr, normed, hid, col,
    local_sem, w_sem, x_s, x_r, zcw_s, zcw_r, zcc_s, zcc_r, dp_s, dp_r,
    rd_s, rd_r, rcw_s, rcw_r, rcc_s, rcc_r, xr_s, xr_r,
):
    rows, width = cur_ref.shape
    full = width * mp
    units = wg.shape[0]
    pair = dp * rows
    e, m, d = lax.axis_index("expert"), lax.axis_index("mp"), lax.axis_index("dp")
    half = n // 2
    first, second = list(range(mp // 2)), list(range(mp // 2, mp))
    every = list(range(mp))

    def block(offset):
        return lax.rem(e + offset + n, n)

    def part(r):
        return lax.rem(m - r + mp, mp)

    def core(k):
        return lax.rem(d + k, dp)

    up_z, down_z = {"expert": block(1)}, {"expert": block(-1)}

    def remote(src, dst, ss, rs, dev):
        return pltpu.make_async_remote_copy(
            src_ref=src, dst_ref=dst, send_sem=ss, recv_sem=rs, device_id=dev, device_id_type=MESH
        )

    sent = []

    def send(copy):
        copy.start()
        sent.append(copy)

    def travels(j, going_up):
        if 2 * j == n:
            return first if going_up else second
        return every

    weights = []
    for i, (src, dst) in enumerate(((wg_hbm, wg), (wu_hbm, wu), (wd_hbm, wd))):
        copy = pltpu.make_async_copy(src.at[layer_idx, 0], dst, w_sem.at[i])
        copy.start()
        weights.append(copy)
    mine = pltpu.make_async_copy(cur_ref, x.at[e, d, m], local_sem.at[0])
    mine.start()

    barrier = pltpu.get_barrier_semaphore()
    peers = [{"mp": part(r)} for r in range(1, mp)] + [up_z, down_z]
    peers += [{"dp": core(k)} for k in range(1, dp)]
    for dev in peers:
        pl.semaphore_signal(barrier, inc=1, device_id=dev, device_id_type=MESH)
    pl.semaphore_wait(barrier, len(peers))
    mine.wait()

    def cw(j, r, blk):
        ref = x.at[blk, d, part(r)]
        return remote(ref, ref, zcw_s.at[j, r], zcw_r.at[j, r], up_z)

    def cc(j, r, blk):
        ref = x.at[blk, d, part(r)]
        return remote(ref, ref, zcc_s.at[j, r], zcc_r.at[j, r], down_z)

    def to_core(level_slot, r, blk):
        for k in range(1, dp):
            ref = x.at[blk, d, part(r)]
            send(remote(ref, ref, dp_s.at[level_slot, r, k], dp_r.at[level_slot, r, k],
                        {"dp": core(k)}))

    def from_core(level_slot, blk):
        for r in every:
            for k in range(1, dp):
                ref = x.at[blk, core(dp - k), part(r)]
                remote(ref, ref, dp_s.at[level_slot, r, k], dp_r.at[level_slot, r, k],
                       {"dp": core(k)}).wait_recv()

    for r in every:
        if r == 0:
            for q in range(1, mp):
                ref = x.at[e, d, m]
                send(remote(ref, ref, x_s.at[q], x_r.at[q], {"mp": lax.rem(m + q, mp)}))
        else:
            ref = x.at[e, d, part(r)]
            remote(ref, ref, x_s.at[r], x_r.at[r], {"mp": lax.rem(m + r, mp)}).wait_recv()
        if r in travels(1, True):
            send(cw(1, r, e))
        if r in travels(1, False):
            send(cc(1, r, e))
        to_core(0, r, e)

    def norm(place, blk):
        for c in range(dp):
            base = place * pair + c * rows
            col[base:base + rows, :] = share_ref[blk, c]

            def chunk(i, _):
                at = pl.ds(pl.multiple_of(i * CHUNK, CHUNK), CHUNK)
                total = jnp.zeros((CHUNK, 1), jnp.float32)
                for q in every:
                    v = x[blk, c, q, at, :].astype(jnp.float32)
                    total = total + jnp.sum(v * v, axis=1, keepdims=True)
                inv = lax.rsqrt(total / full + norm_floor)
                to = pl.ds(pl.multiple_of(base + i * CHUNK, CHUNK), CHUNK)
                for q in every:
                    v = x[blk, c, q, at, :].astype(jnp.float32)
                    normed[to, q * width:(q + 1) * width] = (v * inv * gain_ref[q]).astype(
                        jnp.bfloat16
                    )
                return 0

            lax.fori_loop(0, rows // CHUNK, chunk, 0)

    tile = tile_of(units, 256)
    contract = (((1,), (1,)), ((), ()))

    def hidden(start, blocks):
        for place, blk in enumerate(blocks):
            norm(place, blk)
        size = pair * len(blocks)

        def step(t, _):
            at = pl.ds(pl.multiple_of(t * tile, tile), tile)
            a = normed[0:size, :]
            g = lax.dot_general(a, wg[at, :], contract, preferred_element_type=jnp.float32)
            u = lax.dot_general(a, wu[at, :], contract, preferred_element_type=jnp.float32)
            h = g / (1.0 + jnp.exp(-g)) * u * col[0:size, :]
            hid[start:start + size, at] = h.astype(jnp.bfloat16)
            return 0

        if tile == units:
            a = normed[0:size, :]
            g = lax.dot_general(a, wg[...], contract, preferred_element_type=jnp.float32)
            u = lax.dot_general(a, wu[...], contract, preferred_element_type=jnp.float32)
            h = g / (1.0 + jnp.exp(-g)) * u * col[0:size, :]
            hid[start:start + size, :] = h.astype(jnp.bfloat16)
        else:
            lax.fori_loop(0, units // tile, step, 0)

    def level_blocks(j):
        if j == 0:
            return [e]
        if 2 * j == n:
            return [block(j)]
        return [block(-j), block(j)]

    starts, slots, filled, slot = [], [], 0, 0
    for j in range(half + 1):
        starts.append(filled)
        slots.append(slot)
        count = 1 if j == 0 or 2 * j == n else 2
        filled += count * pair
        slot += count

    from_core(0, e)
    weights[0].wait()
    weights[1].wait()
    hidden(0, [e])
    for j in range(1, half + 1):
        blocks = level_blocks(j)
        low, high = slots[j], slots[j] + len(blocks) - 1
        for r in every:
            if r in travels(j, True):
                cw(j, r, block(-j)).wait_recv()
                if j < half and r in travels(j + 1, True):
                    send(cw(j + 1, r, block(-j)))
                to_core(low, r, block(-j))
            if r in travels(j, False):
                cc(j, r, block(j)).wait_recv()
                if j < half and r in travels(j + 1, False):
                    send(cc(j + 1, r, block(j)))
                to_core(high, r, block(j))
        for i, blk in enumerate(blocks):
            from_core(low + i, blk)
        hidden(starts[j], blocks)

    weights[2].wait()
    ctile = tile_of(width, 256)

    def project(start, blocks):
        size = pair * len(blocks)
        for q in every:
            def step(t, _):
                at = pl.ds(pl.multiple_of(t * ctile, ctile), ctile)
                wide = pl.ds(pl.multiple_of(q * width + t * ctile, ctile), ctile)
                y = jnp.dot(hid[start:start + size, :], wd[:, wide],
                            preferred_element_type=jnp.float32).astype(jnp.bfloat16)
                for i, blk in enumerate(blocks):
                    for c in range(dp):
                        base = i * pair + c * rows
                        p[blk, c, q, :, at] = y[base:base + rows]
                return 0

            lax.fori_loop(0, width // ctile, step, 0)

    def add(blk, q, others):
        def chunk(i, _):
            at = pl.ds(pl.multiple_of(i * CHUNK, CHUNK), CHUNK)
            v = p[blk, d, q, at, :].astype(jnp.float32)
            for ref, index in others:
                v = v + ref[index + (at, slice(None))].astype(jnp.float32)
            p[blk, d, q, at, :] = v.astype(jnp.bfloat16)
            return 0

        lax.fori_loop(0, rows // CHUNK, chunk, 0)

    def back_cw(j, r, blk):
        return remote(p.at[blk, d, part(r)], rcw.at[j - 1, r], rcw_s.at[j, r], rcw_r.at[j, r], up_z)

    def back_cc(j, r, blk):
        return remote(p.at[blk, d, part(r)], rcc.at[j - 1, r], rcc_s.at[j, r], rcc_r.at[j, r], down_z)

    def swap(slot, k, blk):
        return remote(p.at[blk, core(k)], rd.at[slot, k - 1], rd_s.at[slot, k], rd_r.at[slot, k],
                      {"dp": core(k)})

    late_first = every[1:] + every[:1]
    x_back = []
    for j in range(half, -1, -1):
        blocks = level_blocks(j)
        project(starts[j], blocks)
        for i, blk in enumerate(blocks):
            for k in range(1, dp):
                send(swap(slots[j] + i, k, blk))
        for i, blk in enumerate(blocks):
            for k in range(1, dp):
                swap(slots[j] + i, k, blk).wait_recv()
        for r in late_first:
            q = part(r)
            for i, blk in enumerate(blocks):
                others = [(rd, (slots[j] + i, k - 1, q)) for k in range(1, dp)]
                upward = j > 0 and (len(blocks) == 1 or i == 1)
                downward = j > 0 and (len(blocks) == 1 or i == 0)
                if j < half and (upward or j == 0) and r in travels(j + 1, True):
                    back_cw(j + 1, r, blk).wait_recv()
                    others.append((rcw, (j, r)))
                if j < half and (downward or j == 0) and r in travels(j + 1, False):
                    back_cc(j + 1, r, blk).wait_recv()
                    others.append((rcc, (j, r)))
                add(blk, q, others)
                if upward and r in travels(j, True):
                    send(back_cw(j, r, blk))
                if downward and r in travels(j, False):
                    send(back_cc(j, r, blk))
                if j == 0 and r > 0:
                    copy = remote(p.at[e, d, q], xr.at[r], xr_s.at[r], xr_r.at[r], {"mp": q})
                    send(copy)
                    x_back.append(copy)
    for copy in x_back:
        copy.wait_recv()

    def last(i, _):
        at = pl.ds(pl.multiple_of(i * CHUNK, CHUNK), CHUNK)
        v = p[e, d, m, at, :].astype(jnp.float32)
        for r in range(1, mp):
            v = v + xr[r, at, :].astype(jnp.float32)
        out_ref[at, :] = (cur_ref[at, :].astype(jnp.float32) + v).astype(jnp.bfloat16)
        return 0

    lax.fori_loop(0, rows // CHUNK, last, 0)
    for copy in sent:
        copy.wait_send()


def layer(layer_idx, n, dp, mp, current, gain, share, w_gate, w_up, w_down):
    rows, width = current.shape
    units, full = w_gate.shape[2:]
    half = n // 2
    bf, dma = jnp.bfloat16, pltpu.SemaphoreType.DMA
    vmem = pl.BlockSpec(memory_space=pltpu.VMEM)
    hbm = pl.BlockSpec(memory_space=pl.ANY)
    return pl.pallas_call(
        functools.partial(layer_kernel, layer_idx, n, dp, mp),
        out_shape=jax.ShapeDtypeStruct((rows, width), bf),
        in_specs=[vmem, vmem, vmem, hbm, hbm, hbm],
        out_specs=vmem,
        scratch_shapes=[
            pltpu.VMEM((units, full), bf),
            pltpu.VMEM((units, full), bf),
            pltpu.VMEM((units, full), bf),
            pltpu.VMEM((n, dp, mp, rows, width), bf),
            pltpu.VMEM((n, dp, mp, rows, width), bf),
            pltpu.VMEM((n, max(dp - 1, 1), mp, rows, width), bf),
            pltpu.VMEM((half, mp, rows, width), bf),
            pltpu.VMEM((half, mp, rows, width), bf),
            pltpu.VMEM((mp, rows, width), bf),
            pltpu.VMEM((2 * dp * rows, full), bf),
            pltpu.VMEM((n * dp * rows, units), bf),
            pltpu.VMEM((2 * dp * rows, 1), jnp.float32),
            dma((1,)), dma((3,)), dma((mp,)), dma((mp,)),
            dma((half + 1, mp)), dma((half + 1, mp)), dma((half + 1, mp)), dma((half + 1, mp)),
            dma((n, mp, dp)), dma((n, mp, dp)), dma((n, dp)), dma((n, dp)),
            dma((half + 1, mp)), dma((half + 1, mp)), dma((half + 1, mp)), dma((half + 1, mp)),
            dma((mp,)), dma((mp,)),
        ],
        compiler_params=pltpu.CompilerParams(
            collective_id=layer_idx, has_side_effects=True, vmem_limit_bytes=67043328
        ),
    )(current, gain, share, w_gate, w_up, w_down)


def body(hidden_in, norm_gain, expert_ids, gate_counts, exit_layer, w_gate, w_up, w_down):
    n, dp, mp = lax.axis_size("expert"), lax.axis_size("dp"), lax.axis_size("mp")
    rows, width = hidden_in.shape
    expert_range = jnp.arange(n, dtype=jnp.int32)
    counts = gate_counts.astype(jnp.float32)
    gate_share = counts / jnp.sum(counts, axis=2, keepdims=True)
    active = exit_layer[None, :] > jnp.arange(LAYERS, dtype=jnp.int32)[:, None]
    matched = (expert_ids[..., None] == expert_range) & active[:, :, None, None]
    share = jnp.sum(jnp.where(matched, gate_share[..., None], jnp.float32(0.0)), axis=2)
    share = lax.all_gather(share, ("expert", "dp"), axis=1, tiled=True)
    share = lax.dynamic_index_in_dim(share, lax.axis_index("expert"), 2, keepdims=True)
    share = share.reshape(LAYERS, n, dp, rows, 1)
    gain = lax.all_gather(norm_gain, "mp", axis=1, tiled=True).astype(jnp.float32)
    gain = gain.reshape(LAYERS, mp, 1, width)
    current = hidden_in
    for layer_idx in range(LAYERS):
        current = layer(
            layer_idx, n, dp, mp, current, gain[layer_idx], share[layer_idx], w_gate, w_up, w_down
        )
    return current


def solution(mesh):
    in_specs = (
        P(("groups", "expert", "dp"), "mp"),
        P(None, "mp"),
        P(None, ("groups", "expert", "dp"), None),
        P(None, ("groups", "expert", "dp"), None),
        P(("groups", "expert", "dp")),
        P(None, "expert", ("mp", "dp"), None),
        P(None, "expert", ("mp", "dp"), None),
        P(None, "expert", ("mp", "dp"), None),
    )
    out_specs = P(("groups", "expert", "dp"), "mp")
    return jax.shard_map(body, mesh=mesh, in_specs=in_specs, out_specs=out_specs, check_vma=False)
```

```python
import functools

import jax
import jax.numpy as jnp
from jax import lax
from jax.experimental import pallas as pl
from jax.experimental.pallas import tpu as pltpu
from jax.sharding import PartitionSpec as P

LAYERS = 2


norm_floor = 0.1
MESH = pl.DeviceIdType.MESH
CHUNK = 16


def tile_of(length, best):
    tile = best
    while tile >= 128:
        if length % tile == 0:
            return tile
        tile //= 2
    return length


def layer_kernel(
    layer_idx, n, dp, mp,
    cur_ref, gain_ref, share_ref, wg_hbm, wu_hbm, wd_hbm, out_ref,
    wg, wu, wd, x, p, rd, rcw, rcc, xr, normed, hid, col, gains, shares,
    local_sem, w_sem, x_s, x_r, zcw_s, zcw_r, zcc_s, zcc_r, dp_s, dp_r,
    sd_s, sd_r, sz_s, sz_r, g_s, g_r, rd_s, rd_r, rcw_s, rcw_r, rcc_s, rcc_r, xr_s, xr_r,
):
    rows, width = cur_ref.shape
    full = width * mp
    units = wg.shape[0]
    pair = dp * rows
    e, m, d = lax.axis_index("expert"), lax.axis_index("mp"), lax.axis_index("dp")
    half = n // 2
    every = list(range(mp))

    def block(offset):
        return lax.rem(e + offset + n, n)

    def part(r):
        return lax.rem(m - r + mp, mp)

    def core(k):
        return lax.rem(d + k, dp)

    up_z, down_z = {"expert": block(1)}, {"expert": block(-1)}

    def remote(src, dst, ss, rs, dev):
        return pltpu.make_async_remote_copy(
            src_ref=src, dst_ref=dst, send_sem=ss, recv_sem=rs, device_id=dev, device_id_type=MESH
        )

    sent = []

    def send(copy):
        copy.start()
        sent.append(copy)

    weights = []
    for i, (src, dst) in enumerate(((wg_hbm, wg), (wu_hbm, wu), (wd_hbm, wd))):
        copy = pltpu.make_async_copy(src.at[layer_idx, 0], dst, w_sem.at[i])
        copy.start()
        weights.append(copy)
    mine = pltpu.make_async_copy(cur_ref, x.at[e, d, m], local_sem.at[0])
    mine.start()
    own_gain = pltpu.make_async_copy(gain_ref, gains.at[m], local_sem.at[1])
    own_gain.start()
    own_share = pltpu.make_async_copy(share_ref, shares.at[e, d], local_sem.at[2])
    own_share.start()

    barrier = pltpu.get_barrier_semaphore()
    peers = [{"mp": part(r)} for r in range(1, mp)] + [{"expert": block(k)} for k in range(1, n)]
    peers += [{"dp": core(k)} for k in range(1, dp)]
    for dev in peers:
        pl.semaphore_signal(barrier, inc=1, device_id=dev, device_id_type=MESH)
    pl.semaphore_wait(barrier, len(peers))
    mine.wait()
    own_gain.wait()
    own_share.wait()

    def piece(ref, j, going_up):
        if 2 * j == n:
            return ref.at[pl.ds(0 if going_up else rows // 2, rows // 2)]
        return ref

    def cw(j, blk):
        ref = piece(x.at[blk, d, m], j, True)
        return remote(ref, ref, zcw_s.at[j], zcw_r.at[j], up_z)

    def cc(j, blk):
        ref = piece(x.at[blk, d, m], j, False)
        return remote(ref, ref, zcc_s.at[j], zcc_r.at[j], down_z)

    def to_core(slot, r, blk):
        for k in range(1, dp):
            ref = x.at[blk, d, part(r)]
            send(remote(ref, ref, dp_s.at[slot, r, k], dp_r.at[slot, r, k], {"dp": core(k)}))

    def from_core(slot, blk):
        for k in range(1, dp):
            for r in every:
                ref = x.at[blk, core(dp - k), part(r)]
                remote(ref, ref, dp_s.at[slot, r, k], dp_r.at[slot, r, k],
                       {"dp": core(k)}).wait_recv()
            ref = shares.at[blk, core(dp - k)]
            remote(ref, ref, sd_s.at[slot, k], sd_r.at[slot, k], {"dp": core(k)}).wait_recv()

    def to_mp(slot, blk):
        for r in range(1, mp):
            ref = x.at[blk, d, m]
            send(remote(ref, ref, x_s.at[slot, r], x_r.at[slot, r], {"mp": lax.rem(m + r, mp)}))

    def from_mp(slot, blk):
        for r in range(1, mp):
            ref = x.at[blk, d, part(r)]
            remote(ref, ref, x_s.at[slot, r], x_r.at[slot, r],
                   {"mp": lax.rem(m + r, mp)}).wait_recv()
            to_core(slot, r, blk)

    def share_core(slot, blk):
        for k in range(1, dp):
            ref = shares.at[blk, d]
            send(remote(ref, ref, sd_s.at[slot, k], sd_r.at[slot, k], {"dp": core(k)}))

    def level_blocks(j):
        if j == 0:
            return [e]
        if 2 * j == n:
            return [block(j)]
        return [block(-j), block(j)]

    starts, slots, filled, slot = [], [], 0, 0
    for j in range(half + 1):
        starts.append(filled)
        slots.append(slot)
        count = 1 if j == 0 or 2 * j == n else 2
        filled += count * pair
        slot += count

    for r in range(1, mp):
        ref = gains.at[m]
        send(remote(ref, ref, g_s.at[r], g_r.at[r], {"mp": lax.rem(m + r, mp)}))
    for k in range(1, n):
        ref = shares.at[e, d]
        send(remote(ref, ref, sz_s.at[k], sz_r.at[k], {"expert": block(k)}))
    to_mp(0, e)
    send(cw(1, e))
    send(cc(1, e))
    share_core(0, e)
    to_core(0, 0, e)

    def arrive(j):
        blocks = level_blocks(j)
        low, high = slots[j], slots[j] + len(blocks) - 1
        cw(j, block(-j)).wait_recv()
        if j < half:
            send(cw(j + 1, block(-j)))
        if low != high:
            to_mp(low, block(-j))
            to_core(low, 0, block(-j))
        cc(j, block(j)).wait_recv()
        if j < half:
            send(cc(j + 1, block(j)))
        to_mp(high, block(j))
        to_core(high, 0, block(j))

    for r in range(1, mp):
        ref = gains.at[part(r)]
        remote(ref, ref, g_s.at[r], g_r.at[r], {"mp": lax.rem(m + r, mp)}).wait_recv()

    def shares_from(j):
        for i, blk in enumerate(level_blocks(j)):
            k = (j if i == 0 else n - j)
            ref = shares.at[blk, d]
            remote(ref, ref, sz_s.at[k], sz_r.at[k], {"expert": block(k)}).wait_recv()
            share_core(slots[j] + i, blk)

    def norm(place, blk):
        for c in range(dp):
            base = place * pair + c * rows
            lanes = lax.broadcasted_iota(jnp.int32, (rows, shares.shape[3]), 1)
            picked = jnp.where(lanes == e, shares[blk, c], 0.0)
            col[base:base + rows, :] = jnp.sum(picked, axis=1, keepdims=True)

            def chunk(i, _):
                at = pl.ds(pl.multiple_of(i * CHUNK, CHUNK), CHUNK)
                total = jnp.zeros((CHUNK, 1), jnp.float32)
                for q in every:
                    v = x[blk, c, q, at, :].astype(jnp.float32)
                    total = total + jnp.sum(v * v, axis=1, keepdims=True)
                inv = lax.rsqrt(total / full + norm_floor)
                to = pl.ds(pl.multiple_of(base + i * CHUNK, CHUNK), CHUNK)
                for q in every:
                    v = x[blk, c, q, at, :].astype(jnp.float32)
                    normed[to, q * width:(q + 1) * width] = (v * inv * gains[q]).astype(
                        jnp.bfloat16
                    )
                return 0

            lax.fori_loop(0, rows // CHUNK, chunk, 0)

    tile = tile_of(units, 256)
    contract = (((1,), (1,)), ((), ()))

    def hidden(start, blocks):
        for place, blk in enumerate(blocks):
            norm(place, blk)
        size = pair * len(blocks)

        def step(t, _):
            at = pl.ds(pl.multiple_of(t * tile, tile), tile)
            a = normed[0:size, :]
            g = lax.dot_general(a, wg[at, :], contract, preferred_element_type=jnp.float32)
            u = lax.dot_general(a, wu[at, :], contract, preferred_element_type=jnp.float32)
            h = g / (1.0 + jnp.exp(-g)) * u * col[0:size, :]
            hid[start:start + size, at] = h.astype(jnp.bfloat16)
            return 0

        if tile == units:
            a = normed[0:size, :]
            g = lax.dot_general(a, wg[...], contract, preferred_element_type=jnp.float32)
            u = lax.dot_general(a, wu[...], contract, preferred_element_type=jnp.float32)
            h = g / (1.0 + jnp.exp(-g)) * u * col[0:size, :]
            hid[start:start + size, :] = h.astype(jnp.bfloat16)
        else:
            lax.fori_loop(0, units // tile, step, 0)

    from_mp(0, e)
    arrive(1)
    from_core(0, e)
    weights[0].wait()
    weights[1].wait()
    hidden(0, [e])
    for j in range(1, half + 1):
        if j < half:
            arrive(j + 1)
        blocks = level_blocks(j)
        shares_from(j)
        for i, blk in enumerate(blocks):
            from_mp(slots[j] + i, blk)
        for i, blk in enumerate(blocks):
            from_core(slots[j] + i, blk)
        hidden(starts[j], blocks)

    weights[2].wait()
    ctile = tile_of(width, 256)

    def project(start, blocks):
        size = pair * len(blocks)
        for q in every:
            def step(t, _):
                at = pl.ds(pl.multiple_of(t * ctile, ctile), ctile)
                wide = pl.ds(pl.multiple_of(q * width + t * ctile, ctile), ctile)
                y = jnp.dot(hid[start:start + size, :], wd[:, wide],
                            preferred_element_type=jnp.float32).astype(jnp.bfloat16)
                for i, blk in enumerate(blocks):
                    for c in range(dp):
                        base = i * pair + c * rows
                        p[blk, c, q, :, at] = y[base:base + rows]
                return 0

            lax.fori_loop(0, width // ctile, step, 0)

    def add(blk, q, others, begin=0, count=rows):
        def chunk(i, _):
            at = pl.ds(pl.multiple_of(begin + i * CHUNK, CHUNK), CHUNK)
            v = p[blk, d, q, at, :].astype(jnp.float32)
            for ref, index in others:
                v = v + ref[index + (at, slice(None))].astype(jnp.float32)
            p[blk, d, q, at, :] = v.astype(jnp.bfloat16)
            return 0

        lax.fori_loop(0, count // CHUNK, chunk, 0)

    def back_cw(j, blk):
        return remote(piece(p.at[blk, d, m], j, True), piece(rcw.at[j - 1], j, True),
                      rcw_s.at[j], rcw_r.at[j], up_z)

    def back_cc(j, blk):
        return remote(piece(p.at[blk, d, m], j, False), piece(rcc.at[j - 1], j, False),
                      rcc_s.at[j], rcc_r.at[j], down_z)

    def swap(slot, k, blk):
        return remote(p.at[blk, core(k)], rd.at[slot, k - 1], rd_s.at[slot, k], rd_r.at[slot, k],
                      {"dp": core(k)})

    def back_mp(slot, r, blk):
        return remote(p.at[blk, d, part(r)], xr.at[slot, r - 1], xr_s.at[slot, r],
                      xr_r.at[slot, r], {"mp": part(r)})

    def across(j):
        blocks = level_blocks(j)
        project(starts[j], blocks)
        for i, blk in enumerate(blocks):
            for k in range(1, dp):
                send(swap(slots[j] + i, k, blk))
        for i, blk in enumerate(blocks):
            for k in range(1, dp):
                swap(slots[j] + i, k, blk).wait_recv()
            for r in range(1, mp):
                q = part(r)
                add(blk, q, [(rd, (slots[j] + i, k - 1, q)) for k in range(1, dp)])
                send(back_mp(slots[j] + i, r, blk))

    across(half)
    for j in range(half, -1, -1):
        if j > 0:
            across(j - 1)
        blocks = level_blocks(j)
        for i, blk in enumerate(blocks):
            upward = j > 0 and (len(blocks) == 1 or i == 1)
            downward = j > 0 and (len(blocks) == 1 or i == 0)
            others = [(rd, (slots[j] + i, k - 1, m)) for k in range(1, dp)]
            for r in range(1, mp):
                back_mp(slots[j] + i, r, blk).wait_recv()
                others.append((xr, (slots[j] + i, r - 1)))
            add(blk, m, others)
            if j < half and (upward or j == 0):
                back_cw(j + 1, blk).wait_recv()
                split = 2 * (j + 1) == n
                add(blk, m, [(rcw, (j,))], 0, rows // 2 if split else rows)
            if j < half and (downward or j == 0):
                back_cc(j + 1, blk).wait_recv()
                split = 2 * (j + 1) == n
                add(blk, m, [(rcc, (j,))], rows // 2 if split else 0,
                    rows // 2 if split else rows)
            if upward:
                send(back_cw(j, blk))
            if downward:
                send(back_cc(j, blk))

    def last(i, _):
        at = pl.ds(pl.multiple_of(i * CHUNK, CHUNK), CHUNK)
        v = p[e, d, m, at, :].astype(jnp.float32)
        out_ref[at, :] = (cur_ref[at, :].astype(jnp.float32) + v).astype(jnp.bfloat16)
        return 0

    lax.fori_loop(0, rows // CHUNK, last, 0)
    for copy in sent:
        copy.wait_send()


def layer(layer_idx, n, dp, mp, current, gain, share, w_gate, w_up, w_down):
    rows, width = current.shape
    units, full = w_gate.shape[2:]
    half = n // 2
    bf, dma = jnp.bfloat16, pltpu.SemaphoreType.DMA
    vmem = pl.BlockSpec(memory_space=pltpu.VMEM)
    hbm = pl.BlockSpec(memory_space=pl.ANY)
    return pl.pallas_call(
        functools.partial(layer_kernel, layer_idx, n, dp, mp),
        out_shape=jax.ShapeDtypeStruct((rows, width), bf),
        in_specs=[vmem, vmem, vmem, hbm, hbm, hbm],
        out_specs=vmem,
        scratch_shapes=[
            pltpu.VMEM((units, full), bf),
            pltpu.VMEM((units, full), bf),
            pltpu.VMEM((units, full), bf),
            pltpu.VMEM((n, dp, mp, rows, width), bf),
            pltpu.VMEM((n, dp, mp, rows, width), bf),
            pltpu.VMEM((n, max(dp - 1, 1), mp, rows, width), bf),
            pltpu.VMEM((half, rows, width), bf),
            pltpu.VMEM((half, rows, width), bf),
            pltpu.VMEM((n, max(mp - 1, 1), rows, width), bf),
            pltpu.VMEM((2 * dp * rows, full), bf),
            pltpu.VMEM((n * dp * rows, units), bf),
            pltpu.VMEM((2 * dp * rows, 1), jnp.float32),
            pltpu.VMEM((mp, 1, width), jnp.float32),
            pltpu.VMEM((n, dp, rows, share.shape[1]), jnp.float32),
            dma((3,)), dma((3,)), dma((n, mp)), dma((n, mp)),
            dma((half + 1,)), dma((half + 1,)), dma((half + 1,)), dma((half + 1,)),
            dma((n, mp, dp)), dma((n, mp, dp)),
            dma((n, dp)), dma((n, dp)), dma((n,)), dma((n,)), dma((mp,)), dma((mp,)),
            dma((n, dp)), dma((n, dp)),
            dma((half + 1,)), dma((half + 1,)), dma((half + 1,)), dma((half + 1,)),
            dma((n, mp)), dma((n, mp)),
        ],
        compiler_params=pltpu.CompilerParams(
            collective_id=layer_idx, has_side_effects=True, vmem_limit_bytes=67043328
        ),
    )(current, gain, share, w_gate, w_up, w_down)


def body(hidden_in, norm_gain, expert_ids, gate_counts, exit_layer, w_gate, w_up, w_down):
    n, dp, mp = lax.axis_size("expert"), lax.axis_size("dp"), lax.axis_size("mp")
    rows, width = hidden_in.shape
    expert_range = jnp.arange(n, dtype=jnp.int32)
    counts = gate_counts.astype(jnp.float32)
    gate_share = counts / jnp.sum(counts, axis=2, keepdims=True)
    active = exit_layer[None, :] > jnp.arange(LAYERS, dtype=jnp.int32)[:, None]
    matched = (expert_ids[..., None] == expert_range) & active[:, :, None, None]
    share = jnp.sum(jnp.where(matched, gate_share[..., None], jnp.float32(0.0)), axis=2)
    share = jnp.pad(share, ((0, 0), (0, 0), (0, -n % 128)))
    gain = norm_gain.astype(jnp.float32)[:, None, :]
    current = hidden_in
    for layer_idx in range(LAYERS):
        current = layer(
            layer_idx, n, dp, mp, current, gain[layer_idx], share[layer_idx], w_gate, w_up, w_down
        )
    return current


def solution(mesh):
    in_specs = (
        P(("groups", "expert", "dp"), "mp"),
        P(None, "mp"),
        P(None, ("groups", "expert", "dp"), None),
        P(None, ("groups", "expert", "dp"), None),
        P(("groups", "expert", "dp")),
        P(None, "expert", ("mp", "dp"), None),
        P(None, "expert", ("mp", "dp"), None),
        P(None, "expert", ("mp", "dp"), None),
    )
    out_specs = P(("groups", "expert", "dp"), "mp")
    return jax.shard_map(body, mesh=mesh, in_specs=in_specs, out_specs=out_specs, check_vma=False)
```
